32 devices in a mesh: dp: 1 (over z), ri: 4 (over y), co: 4 (over x), ro: 2 (over core).
Axes of the slice: x: 4, y: 4, z: 1, core: 2. Of those that a mesh axis runs over, the one named last changes fastest.
The devices are a block of a 4x4x8 slice.
Arguments:
- act_in: bfloat16 [32768, 4096], P(('dp', 'ro', 'ri'), 'co')
- weight: bfloat16 [4096, 14336], P(('ro', 'ri'), 'co')
Outputs:
- output: bfloat16 [32768, 14336], P(('dp', 'ro', 'ri', 'co'))
All inputs are finite; a program needn't handle non-finite values.
Results may differ from the reference program's by a relative error of at most 0.001.
Values are sent between devices in bfloat16 or wider.
A program may use at most 768 MiB of HBM per device.

```python
import jax
import jax.numpy as jnp

ROWS_TOTAL = 32768
D_IN = 4096
D_OUT = 14336


def setup_inputs(seed: int = 0, part: int = 0) -> dict:
    key = jax.random.key(seed)
    key_a = jax.random.fold_in(jax.random.fold_in(key, 1), part)
    key_b = jax.random.fold_in(key, 2)
    act_in = jax.random.normal(key_a, (ROWS_TOTAL, D_IN), jnp.float32)
    weight = jax.random.normal(key_b, (D_IN, D_OUT), jnp.float32) * (D_IN ** -0.5)
    return {"act_in": act_in.astype(jnp.bfloat16), "weight": weight.astype(jnp.bfloat16)}


def reference(act_in, weight):
    product = jnp.dot(act_in, weight, preferred_element_type=jnp.float32)
    return product.astype(jnp.bfloat16)
```

```python
import functools

import jax
import jax.numpy as jnp
from jax import lax
from jax.experimental import pallas as pl
from jax.experimental.pallas import tpu as pltpu
from jax.sharding import PartitionSpec as P

MESH = pl.DeviceIdType.MESH
LANES = 128
A_PIECES = 8
P1L, P1R, P1O, P2L, P2R, P2O, Q1L, Q1R, Q1O, Q2L, Q2R, Q2O, DIE = range(13)


def kernel(dims, act, w, out, g, a_v, w_v, b_v, c_v, rsem, ssem, a_rsem, a_ssem, lsem, bsem, csem):
    nx, ny = dims
    kb, wcols = w.shape
    n = wcols // LANES
    full = n // 4
    half = kb // 2
    rows, kd = a_v.shape
    acols = kd // nx
    apiece = rows // A_PIECES

    x, y, c = lax.axis_index("co"), lax.axis_index("ri"), lax.axis_index("ro")
    xl, xr, xo = lax.rem(x + nx - 1, nx), lax.rem(x + 1, nx), lax.rem(x + 2, nx)
    yl, yr = lax.rem(y + ny - 1, ny), lax.rem(y + 1, ny)

    barrier = pltpu.get_barrier_semaphore()
    peers = [{"co": xl}, {"co": xr}, {"co": xo}, {"ri": yl}, {"ri": yr}, {"ro": 1 - c}]
    for peer in peers:
        pl.semaphore_signal(barrier, inc=1, device_id=peer, device_id_type=MESH)
    pl.semaphore_wait(barrier, len(peers))

    def remote(src, dst, kind, j, dev):
        return pltpu.make_async_remote_copy(
            src_ref=src, dst_ref=dst, send_sem=ssem.at[kind, j], recv_sem=rsem.at[kind, j], device_id=dev, device_id_type=MESH
        )

    def arrived(ref, kind, j):
        remote(ref, ref, kind, j, {"ro": 1 - c}).wait_recv()

    def cols(j):
        return pl.ds(pl.multiple_of(j * LANES, LANES), LANES)

    def prow(is_full):
        return pl.ds(0, kb if is_full else half)

    qrow = pl.ds(half, kb - half)

    def flip(i, m, j):
        odd = lax.rem(j, 2)
        return lax.rem(i + m - 1 + 2 * odd, m), lax.rem(i + 1 + 2 * odd, m)

    def s0p(j, t):
        src, dst = w.at[prow(t), cols(j)], g.at[j, c, y, x, prow(t), :]
        remote(src, dst, P1L, j, {"co": xr}).start()
        remote(src, dst, P1R, j, {"co": xl}).start()

    def s1p(j, t):
        arrived(g.at[j, c, y, xl, prow(t), :], P1L, j)
        arrived(g.at[j, c, y, xr, prow(t), :], P1R, j)
        b, dev = flip(x, nx, j)
        ref = g.at[j, c, y, b, prow(t), :]
        remote(ref, ref, P1O, j, {"co": dev}).start()

    def s2p(j, t):
        arrived(g.at[j, c, y, xo, prow(t), :], P1O, j)
        ref = g.at[j, c, y, :, prow(t), :]
        remote(ref, ref, P2L, j, {"ri": yr}).start()
        remote(ref, ref, P2R, j, {"ri": yl}).start()

    def s3p(j, t):
        arrived(g.at[j, c, yl, :, prow(t), :], P2L, j)
        arrived(g.at[j, c, yr, :, prow(t), :], P2R, j)
        b, dev = flip(y, ny, j)
        ref = g.at[j, c, b, :, prow(t), :]
        remote(ref, ref, P2O, j, {"ri": dev}).start()

    def s4p(j, t):
        arrived(g.at[j, c, y, :, prow(t), :], P2O, j)

    def s0q(j):
        src, dst = w.at[qrow, cols(j)], g.at[j, c, y, x, qrow, :]
        remote(src, dst, Q1L, j, {"ri": yr}).start()
        remote(src, dst, Q1R, j, {"ri": yl}).start()

    def s1q(j):
        arrived(g.at[j, c, yl, x, qrow, :], Q1L, j)
        arrived(g.at[j, c, yr, x, qrow, :], Q1R, j)
        b, dev = flip(y, ny, j)
        ref = g.at[j, c, b, x, qrow, :]
        remote(ref, ref, Q1O, j, {"ri": dev}).start()

    def s2q(j):
        arrived(g.at[j, c, y, x, qrow, :], Q1O, j)
        ref = g.at[j, c, :, x, qrow, :]
        remote(ref, ref, Q2L, j, {"co": xr}).start()
        remote(ref, ref, Q2R, j, {"co": xl}).start()

    def s3q(j):
        arrived(g.at[j, c, :, xl, qrow, :], Q2L, j)
        arrived(g.at[j, c, :, xr, qrow, :], Q2R, j)
        b, dev = flip(x, nx, j)
        ref = g.at[j, c, :, b, qrow, :]
        remote(ref, ref, Q2O, j, {"co": dev}).start()

    def s4q(j):
        arrived(g.at[j, c, :, x, qrow, :], Q2O, j)

    def own(j):
        return pltpu.make_async_copy(w_v.at[:, cols(j)], g.at[j, c, y, x], lsem.at[j])

    def die(j):
        return remote(g.at[j, c], g.at[j, c], DIE, j, {"ro": 1 - c})

    def a_copy(i, k, dev):
        src = act.at[pl.ds(pl.multiple_of(dev * rows + k * apiece, apiece), apiece), :]
        dst = a_v.at[pl.ds(pl.multiple_of(k * apiece, apiece), apiece), pl.ds(pl.multiple_of(x * acols, acols), acols)]
        return pltpu.make_async_remote_copy(
            src_ref=src, dst_ref=dst, send_sem=a_ssem.at[i], recv_sem=a_rsem.at[i], device_id={"co": dev}, device_id_type=MESH
        )

    def a_all(i, src_x):
        ref = a_v.at[:, pl.ds(pl.multiple_of(src_x * acols, acols), acols)]
        return pltpu.make_async_remote_copy(
            src_ref=ref, dst_ref=ref, send_sem=a_ssem.at[i], recv_sem=a_rsem.at[i], device_id={"ro": 1 - c}, device_id_type=MESH
        )

    own_a = pltpu.make_async_copy(
        act.at[pl.ds(pl.multiple_of(x * rows, rows), rows), :], a_v.at[:, pl.ds(pl.multiple_of(x * acols, acols), acols)], lsem.at[n]
    )
    own_w = pltpu.make_async_copy(w, w_v, lsem.at[n + 1])

    def load(j, slot):
        return [
            pltpu.make_async_copy(g.at[j, :, :, i], b_v.at[slot, :, :, :, pl.ds(i * LANES, LANES)], bsem.at[slot, i])
            for i in range(nx)
        ]

    def store(j, slot):
        return [
            pltpu.make_async_copy(
                c_v.at[slot, :, pl.ds(i * LANES, LANES)],
                out.at[:, pl.ds(pl.multiple_of(i * wcols + j * LANES, LANES), LANES)],
                csem.at[slot, i],
            )
            for i in range(nx)
        ]

    def compute(slot):
        def tile(m, _):
            r = pl.ds(pl.multiple_of(m * 256, 256), 256)
            b = b_v[slot].reshape(kd, nx * LANES)
            c_v[slot, r, :] = jnp.dot(a_v[r, :], b, preferred_element_type=jnp.float32).astype(c_v.dtype)
            return 0

        lax.fori_loop(0, rows // 256, tile, 0)

    def step(i, _):
        slot = lax.rem(i, 2)

        @pl.when(i == 0)
        def _():
            own_a.wait()
            a_all(0, xl).wait_recv()
            a_all(1, xr).wait_recv()
            a_all(2, xo).wait_recv()

        @pl.when(i < n)
        def _():
            arrived(g.at[i, 1 - c], DIE, i)
            for cp in load(i, slot):
                cp.start()

        @pl.when(i >= 1)
        def _():
            for cp in load(i - 1, 1 - slot):
                cp.wait()

            @pl.when(i >= 3)
            def _():
                for cp in store(i - 3, 1 - slot):
                    cp.wait()

            compute(1 - slot)
            for cp in store(i - 1, 1 - slot):
                cp.start()

        return 0

    def by_type(j, stage):
        pl.when((j >= 0) & (j < full))(lambda: stage(j, True))
        pl.when((j >= full) & (j < n))(lambda: stage(j, False))

    def if_q(j, stage):
        pl.when((j >= full) & (j < n))(lambda: stage(j))

    own_w.start()
    own_a.start()
    own_w.wait()

    def start_own(j, _):
        own(j).start()
        return 0

    lead = 6
    c_start = 7

    def progress(r):
        return jnp.clip(jnp.minimum(2 * (r - c_start), r - 3), 0, n + 1)

    def turn(t, _):
        r = t - lead
        by_type(r + 6, s0p)
        if_q(r + full + 6, s0q)

        @pl.when(t == 0)
        def _():
            lax.fori_loop(0, n, start_own, 0)

        by_type(r + 4, s1p)
        if_q(r + full + 4, s1q)

        @pl.when((r >= -3) & (r < A_PIECES - 3))
        def _():
            for i, dev in enumerate((xr, xl, xo)):
                a_copy(i, r + 3, dev).start()

        @pl.when((r + 2 >= 0) & (r + 2 < n))
        def _():
            own(r + 2).wait()

        by_type(r + 2, s2p)
        if_q(r + 2, s2q)
        by_type(r, s3p)
        if_q(r, s3q)
        by_type(r - 2, s4p)
        if_q(r - 2, s4q)
        pl.when((r - 2 >= 0) & (r - 2 < n))(lambda: die(r - 2).start())
        lax.fori_loop(progress(r), progress(r + 1), step, 0)
        return 0

    lax.fori_loop(0, n + 4 + lead, turn, 0)

    for j in (n - 2, n - 1):
        for cp in store(j, j % 2):
            cp.wait()
    for i, src_x in enumerate((xl, xr, xo)):
        a_all(i, src_x).wait_send()

    def sent(j, _):
        def p(j, t):
            one, four = g.at[j, c, y, x, prow(t), :], g.at[j, c, y, :, prow(t), :]
            for kind in (P1L, P1R, P1O):
                remote(one, one, kind, j, {"ro": 1 - c}).wait_send()
            for kind in (P2L, P2R, P2O):
                remote(four, four, kind, j, {"ro": 1 - c}).wait_send()

        def q(j):
            one, four = g.at[j, c, y, x, qrow, :], g.at[j, c, :, x, qrow, :]
            for kind in (Q1L, Q1R, Q1O):
                remote(one, one, kind, j, {"ro": 1 - c}).wait_send()
            for kind in (Q2L, Q2R, Q2O):
                remote(four, four, kind, j, {"ro": 1 - c}).wait_send()

        by_type(j, p)
        if_q(j, q)
        die(j).wait_send()
        return 0

    lax.fori_loop(0, n, sent, 0)


def solution(mesh):
    nx, ny, nc = mesh.shape["co"], mesh.shape["ri"], mesh.shape["ro"]

    def local_block(act, w):
        kb, wcols = w.shape
        n = wcols // LANES
        rows, kd = act.shape[0] // nx, act.shape[1] * nx
        dt = act.dtype
        out, _ = pl.pallas_call(
            functools.partial(kernel, (nx, ny)),
            name="gather_matmul",
            out_shape=(
                jax.ShapeDtypeStruct((rows, wcols * nx), dt),
                jax.ShapeDtypeStruct((n, nc, ny, nx, kb, LANES), dt),
            ),
            in_specs=[pl.BlockSpec(memory_space=pl.ANY)] * 2,
            out_specs=(pl.BlockSpec(memory_space=pl.ANY),) * 2,
            scratch_shapes=[
                pltpu.VMEM((rows, kd), dt),
                pltpu.VMEM((kb, wcols), dt),
                pltpu.VMEM((2, nc, ny, kb, nx * LANES), dt),
                pltpu.VMEM((2, rows, nx * LANES), dt),
                pltpu.SemaphoreType.DMA((13, n)),
                pltpu.SemaphoreType.DMA((13, n)),
                pltpu.SemaphoreType.DMA((3,)),
                pltpu.SemaphoreType.DMA((3,)),
                pltpu.SemaphoreType.DMA((n + 2,)),
                pltpu.SemaphoreType.DMA((2, nx)),
                pltpu.SemaphoreType.DMA((2, nx)),
            ],
            compiler_params=pltpu.CompilerParams(collective_id=0, has_side_effects=True, vmem_limit_bytes=60 << 20),
        )(act, w)
        return out

    return jax.shard_map(
        local_block,
        mesh=mesh,
        in_specs=(P(("dp", "ro", "ri"), "co"), P(("ro", "ri"), "co")),
        out_specs=P(("dp", "ro", "ri", "co"), None),
        check_vma=False,
    )
```

```python
import functools

import jax
import jax.numpy as jnp
from jax import lax
from jax.experimental import pallas as pl
from jax.experimental.pallas import tpu as pltpu
from jax.sharding import PartitionSpec as P

MESH = pl.DeviceIdType.MESH
LANES = 128
A_PIECES = 8
FIN = 2
TILE = 512
C_PARTS = 8
P1L, P1R, P1U, P1D, P2L, P2R, P2U, P2D, Q1L, Q1R, Q1U, Q1D, Q2L, Q2R, Q2U, Q2D, DIE = range(17)


def kernel(dims, act, w, a_v, b_v, c_v, g, w_v, rsem, ssem, a_rsem, a_ssem, lsem, bsem):
    nx, ny = dims
    kb, wcols = w.shape
    n = wcols // LANES
    nc = n - FIN
    full = n // 4
    half = kb // 2
    rows, kd = a_v.shape
    acols = kd // nx
    apiece = rows // A_PIECES

    x, y, c = lax.axis_index("co"), lax.axis_index("ri"), lax.axis_index("ro")
    xl, xr, xo = lax.rem(x + nx - 1, nx), lax.rem(x + 1, nx), lax.rem(x + 2, nx)
    yl, yr, yo = lax.rem(y + ny - 1, ny), lax.rem(y + 1, ny), lax.rem(y + 2, ny)

    barrier = pltpu.get_barrier_semaphore()
    peers = [{"co": xl}, {"co": xr}, {"co": xo}, {"ri": yl}, {"ri": yr}, {"ro": 1 - c}]
    for peer in peers:
        pl.semaphore_signal(barrier, inc=1, device_id=peer, device_id_type=MESH)
    pl.semaphore_wait(barrier, len(peers))

    def remote(src, dst, kind, j, dev):
        return pltpu.make_async_remote_copy(
            src_ref=src, dst_ref=dst, send_sem=ssem.at[kind, j], recv_sem=rsem.at[kind, j], device_id=dev, device_id_type=MESH
        )

    def arrived(ref, kind, j):
        remote(ref, ref, kind, j, {"ro": 1 - c}).wait_recv()

    def cols(j):
        return pl.ds(pl.multiple_of(j * LANES, LANES), LANES)

    def prow(is_full, part=0):
        size = kb if is_full else half
        return (pl.ds(0, size), pl.ds(0, size // 2), pl.ds(size // 2, size // 2))[part]

    def qrow(part=0):
        size = kb - half
        return (pl.ds(half, size), pl.ds(half, size // 2), pl.ds(half + size // 2, size // 2))[part]

    def s0p(j, t):
        src, dst = w.at[prow(t), cols(j)], g.at[j, c, y, x, prow(t), :]
        remote(src, dst, P1L, j, {"co": xr}).start()
        remote(src, dst, P1R, j, {"co": xl}).start()

    def s1p(j, t):
        arrived(g.at[j, c, y, xl, prow(t), :], P1L, j)
        up = g.at[j, c, y, xl, prow(t, 1), :]
        remote(up, up, P1U, j, {"co": xr}).start()
        arrived(g.at[j, c, y, xr, prow(t), :], P1R, j)
        down = g.at[j, c, y, xr, prow(t, 2), :]
        remote(down, down, P1D, j, {"co": xl}).start()

    def s2p(j, t):
        arrived(g.at[j, c, y, xo, prow(t, 1), :], P1U, j)
        arrived(g.at[j, c, y, xo, prow(t, 2), :], P1D, j)
        ref = g.at[j, c, y, :, prow(t), :]
        remote(ref, ref, P2L, j, {"ri": yr}).start()
        remote(ref, ref, P2R, j, {"ri": yl}).start()

    def s3p(j, t):
        arrived(g.at[j, c, yl, :, prow(t), :], P2L, j)
        up = g.at[j, c, yl, :, prow(t, 1), :]
        remote(up, up, P2U, j, {"ri": yr}).start()
        arrived(g.at[j, c, yr, :, prow(t), :], P2R, j)
        down = g.at[j, c, yr, :, prow(t, 2), :]
        remote(down, down, P2D, j, {"ri": yl}).start()

    def s4p(j, t):
        arrived(g.at[j, c, yo, :, prow(t, 1), :], P2U, j)
        arrived(g.at[j, c, yo, :, prow(t, 2), :], P2D, j)

    def s0q(j):
        src, dst = w.at[qrow(), cols(j)], g.at[j, c, y, x, qrow(), :]
        remote(src, dst, Q1L, j, {"ri": yr}).start()
        remote(src, dst, Q1R, j, {"ri": yl}).start()

    def s1q(j):
        arrived(g.at[j, c, yl, x, qrow(), :], Q1L, j)
        up = g.at[j, c, yl, x, qrow(1), :]
        remote(up, up, Q1U, j, {"ri": yr}).start()
        arrived(g.at[j, c, yr, x, qrow(), :], Q1R, j)
        down = g.at[j, c, yr, x, qrow(2), :]
        remote(down, down, Q1D, j, {"ri": yl}).start()

    def s2q(j):
        arrived(g.at[j, c, yo, x, qrow(1), :], Q1U, j)
        arrived(g.at[j, c, yo, x, qrow(2), :], Q1D, j)
        ref = g.at[j, c, :, x, qrow(), :]
        remote(ref, ref, Q2L, j, {"co": xr}).start()
        remote(ref, ref, Q2R, j, {"co": xl}).start()

    def s3q(j):
        arrived(g.at[j, c, :, xl, qrow(), :], Q2L, j)
        up = g.at[j, c, :, xl, qrow(1), :]
        remote(up, up, Q2U, j, {"co": xr}).start()
        arrived(g.at[j, c, :, xr, qrow(), :], Q2R, j)
        down = g.at[j, c, :, xr, qrow(2), :]
        remote(down, down, Q2D, j, {"co": xl}).start()

    def s4q(j):
        arrived(g.at[j, c, :, xo, qrow(1), :], Q2U, j)
        arrived(g.at[j, c, :, xo, qrow(2), :], Q2D, j)

    def own(j):
        return pltpu.make_async_copy(w_v.at[:, cols(j)], g.at[j, c, y, x], lsem.at[j])

    def die(j):
        return remote(g.at[j, c], g.at[j, c], DIE, j, {"ro": 1 - c})

    def a_copy(i, k, dev):
        src = act.at[pl.ds(pl.multiple_of(dev * rows + k * apiece, apiece), apiece), :]
        dst = a_v.at[pl.ds(pl.multiple_of(k * apiece, apiece), apiece), pl.ds(pl.multiple_of(x * acols, acols), acols)]
        return pltpu.make_async_remote_copy(
            src_ref=src, dst_ref=dst, send_sem=a_ssem.at[i], recv_sem=a_rsem.at[i], device_id={"co": dev}, device_id_type=MESH
        )

    def a_all(i, src_x):
        ref = a_v.at[:, pl.ds(pl.multiple_of(src_x * acols, acols), acols)]
        return pltpu.make_async_remote_copy(
            src_ref=ref, dst_ref=ref, send_sem=a_ssem.at[i], recv_sem=a_rsem.at[i], device_id={"ro": 1 - c}, device_id_type=MESH
        )

    own_a = pltpu.make_async_copy(
        act.at[pl.ds(pl.multiple_of(x * rows, rows), rows), :], a_v.at[:, pl.ds(pl.multiple_of(x * acols, acols), acols)], lsem.at[n]
    )
    own_w = pltpu.make_async_copy(w, w_v, lsem.at[n + 1])

    def load(j, slot):
        return loads(g, b_v, bsem, j, slot)

    def step(i, _):
        slot = lax.rem(i, 2)

        @pl.when(i == 0)
        def _():
            own_a.wait()
            a_all(0, xl).wait_recv()
            a_all(1, xr).wait_recv()
            a_all(2, xo).wait_recv()

        @pl.when(i <= nc)
        def _():
            arrived(g.at[i, 1 - c], DIE, i)
            for cp in load(i, slot):
                cp.start()

        @pl.when(i >= 1)
        def _():
            for cp in load(i - 1, 1 - slot):
                cp.wait()
            multiply(a_v, b_v.at[1 - slot], c_v, i - 1)

        return 0

    def by_type(j, stage):
        pl.when((j >= 0) & (j < full))(lambda: stage(j, True))
        pl.when((j >= full) & (j < n))(lambda: stage(j, False))

    def if_q(j, stage):
        pl.when((j >= full) & (j < n))(lambda: stage(j))

    own_w.start()
    own_a.start()

    def start_own(j, _):
        own(j).start()
        return 0

    gap = 3
    lead = 3 * gap
    c_start = 7
    a_start = 3

    def finished(r):
        return jnp.clip(jnp.where(r <= n, r - gap, 2 * r - n - gap), 0, n)

    def progress(r):
        return jnp.clip(jnp.minimum(2 * (r - c_start), r - gap - 1), 0, nc + 1)

    def last_hop(j, _):
        by_type(j, s4p)
        if_q(j, s4q)

        @pl.when(j < n - 1)
        def _():
            die(j).start()

        @pl.when(j == n - 1)
        def _():
            die_part(g.at[j, c, yo, :, prow(False), :]).start()
            die_part(g.at[j, c, :, xo, qrow(), :]).start()

        return 0

    def die_part(ref):
        return remote(ref, ref, DIE, n - 1, {"ro": 1 - c})

    def turn(t, _):
        r = t - lead
        by_type(r + 3 * gap, s0p)
        if_q(r + full + 3 * gap, s0q)

        @pl.when(t == 0)
        def _():
            own_w.wait()
            lax.fori_loop(0, n, start_own, 0)

        by_type(r + 2 * gap, s1p)
        if_q(r + full + 2 * gap, s1q)

        @pl.when((r >= -a_start) & (r < A_PIECES - a_start))
        def _():
            for i, dev in enumerate((xr, xl, xo)):
                a_copy(i, r + a_start, dev).start()

        @pl.when((r + gap >= 0) & (r + gap < n))
        def _():
            own(r + gap).wait()

        by_type(r + gap, s2p)
        if_q(r + gap, s2q)
        j3 = jnp.where(r == n - 1, n, jnp.where(r == n, n - 1, r))
        by_type(j3, s3p)
        if_q(j3, s3q)

        @pl.when(j3 == n - 1)
        def _():
            for b in (y, yl, yr):
                die_part(g.at[j3, c, b, :, prow(False), :]).start()
            for b in (x, xl, xr):
                die_part(g.at[j3, c, :, b, qrow(), :]).start()

        lax.fori_loop(finished(r), finished(r + 1), last_hop, 0)
        lax.fori_loop(progress(r), progress(r + 1), step, 0)
        return 0

    lax.fori_loop(0, nc + gap + 2 + lead, turn, 0)

    for cp in load(nc, nc % 2):
        cp.wait()
    arrived(g.at[n - 1, 1 - c], DIE, n - 1)
    for i, src_x in enumerate((xl, xr, xo)):
        a_all(i, src_x).wait_send()

    def sent(j, _):
        def p(j, t):
            for kind, ref in (
                (P1L, g.at[j, c, y, x, prow(t), :]),
                (P1R, g.at[j, c, y, x, prow(t), :]),
                (P1U, g.at[j, c, y, x, prow(t, 1), :]),
                (P1D, g.at[j, c, y, x, prow(t, 2), :]),
                (P2L, g.at[j, c, y, :, prow(t), :]),
                (P2R, g.at[j, c, y, :, prow(t), :]),
                (P2U, g.at[j, c, y, :, prow(t, 1), :]),
                (P2D, g.at[j, c, y, :, prow(t, 2), :]),
            ):
                remote(ref, ref, kind, j, {"ro": 1 - c}).wait_send()

        def q(j):
            for kind, ref in (
                (Q1L, g.at[j, c, y, x, qrow(), :]),
                (Q1R, g.at[j, c, y, x, qrow(), :]),
                (Q1U, g.at[j, c, y, x, qrow(1), :]),
                (Q1D, g.at[j, c, y, x, qrow(2), :]),
                (Q2L, g.at[j, c, :, x, qrow(), :]),
                (Q2R, g.at[j, c, :, x, qrow(), :]),
                (Q2U, g.at[j, c, :, x, qrow(1), :]),
                (Q2D, g.at[j, c, :, x, qrow(2), :]),
            ):
                remote(ref, ref, kind, j, {"ro": 1 - c}).wait_send()

        by_type(j, p)
        if_q(j, q)
        die(j).wait_send()
        return 0

    lax.fori_loop(0, n, sent, 0)


def loads(g, b_v, sem, j, slot):
    return [
        pltpu.make_async_copy(g.at[j, :, :, i], b_v.at[slot, :, :, :, pl.ds(i * LANES, LANES)], sem.at[slot, i])
        for i in range(g.shape[3])
    ]


def multiply(a_v, b, c_v, j):
    nx = b.shape[-1] // LANES
    width = c_v.shape[-1] // nx

    def tile(m, _):
        r = pl.ds(pl.multiple_of(m * TILE, TILE), TILE)
        c = jnp.dot(a_v[r, :], b[...].reshape(a_v.shape[-1], nx * LANES), preferred_element_type=jnp.float32)
        for i in range(nx):
            col = pl.ds(pl.multiple_of(i * width + j * LANES, LANES), LANES)
            c_v[r, col] = c[:, i * LANES : (i + 1) * LANES].astype(c_v.dtype)
        return 0

    lax.fori_loop(0, a_v.shape[0] // TILE, tile, 0)


def finish(a_v, b_v, c_v, g, out, last_v, d_v, bsem, csem, dsem):
    n, _, _, nx, _, _ = g.shape
    rows, nc = c_v.shape[0], n - FIN
    part = rows // C_PARTS

    def stores(ref, first, count, sem):
        width = count * LANES
        cps = []
        for k in range(C_PARTS):
            for i in range(nx):
                r = pl.ds(k * part, part)
                dst = out.at[r, pl.ds(i * n * LANES + first * LANES, width)]
                cps.append(pltpu.make_async_copy(ref.at[r, pl.ds(i * width, width)], dst, sem.at[k, i]))
        return cps

    for cp in loads(g, last_v, bsem, n - 1, 0):
        cp.start()
    for cp in stores(c_v, 0, nc, csem):
        cp.start()

    multiply(a_v, b_v.at[nc % 2], d_v, 0)
    for cp in loads(g, last_v, bsem, n - 1, 0):
        cp.wait()
    multiply(a_v, last_v.at[0], d_v, 1)
    for cp in stores(d_v, nc, FIN, dsem):
        cp.start()
    for cp in stores(c_v, 0, nc, csem) + stores(d_v, nc, FIN, dsem):
        cp.wait()


def solution(mesh):
    nx, ny, ncore = mesh.shape["co"], mesh.shape["ri"], mesh.shape["ro"]

    def local_block(act, w):
        kb, wcols = w.shape
        n = wcols // LANES
        rows, kd = act.shape[0] // nx, act.shape[1] * nx
        dt = act.dtype
        wide = nx * LANES
        any_spec = pl.BlockSpec(memory_space=pl.ANY)
        vmem_spec = pl.BlockSpec(memory_space=pltpu.VMEM)
        a_v, b_v, c_v, g = pl.pallas_call(
            functools.partial(kernel, (nx, ny)),
            name="gather_matmul",
            out_shape=(
                pltpu.VMEM((rows, kd), dt),
                pltpu.VMEM((2, ncore, ny, kb, wide), dt),
                pltpu.VMEM((rows, wide * (n - FIN)), dt),
                jax.ShapeDtypeStruct((n, ncore, ny, nx, kb, LANES), dt),
            ),
            in_specs=[any_spec] * 2,
            out_specs=(vmem_spec, vmem_spec, vmem_spec, any_spec),
            scratch_shapes=[
                pltpu.VMEM((kb, wcols), dt),
                pltpu.SemaphoreType.DMA((17, n)),
                pltpu.SemaphoreType.DMA((17, n)),
                pltpu.SemaphoreType.DMA((3,)),
                pltpu.SemaphoreType.DMA((3,)),
                pltpu.SemaphoreType.DMA((n + 2,)),
                pltpu.SemaphoreType.DMA((2, nx)),
            ],
            compiler_params=pltpu.CompilerParams(collective_id=0, has_side_effects=True, vmem_limit_bytes=12 << 20),
        )(act, w)
        held = [pltpu.with_memory_space_constraint(v, pltpu.VMEM) for v in (a_v, b_v, c_v)]
        return pl.pallas_call(
            finish,
            name="finish",
            out_shape=jax.ShapeDtypeStruct((rows, wcols * nx), dt),
            in_specs=[vmem_spec] * 3 + [any_spec],
            out_specs=any_spec,
            scratch_shapes=[
                pltpu.VMEM((1, ncore, ny, kb, wide), dt),
                pltpu.VMEM((rows, wide * FIN), dt),
                pltpu.SemaphoreType.DMA((1, nx)),
                pltpu.SemaphoreType.DMA((C_PARTS, nx)),
                pltpu.SemaphoreType.DMA((C_PARTS, nx)),
            ],
            compiler_params=pltpu.CompilerParams(vmem_limit_bytes=12 << 20),
        )(*held, g)

    return jax.shard_map(
        local_block,
        mesh=mesh,
        in_specs=(P(("dp", "ro", "ri"), "co"), P(("ro", "ri"), "co")),
        out_specs=P(("dp", "ro", "ri", "co"), None),
        check_vma=False,
    )
```

```python
import functools

import jax
import jax.numpy as jnp
from jax import lax
from jax.experimental import pallas as pl
from jax.experimental.pallas import tpu as pltpu
from jax.sharding import PartitionSpec as P

MESH = pl.DeviceIdType.MESH
LANES = 128
A_PIECES = 8
FIN = 2
TILE = 512
C_PARTS = 4
P1L, P1R, P1U, P1D, P2L, P2R, P2U, P2D, Q1L, Q1R, Q1U, Q1D, Q2L, Q2R, Q2U, Q2D, DIE = range(17)


def kernel(dims, act, w, a_v, b_v, c_v, g, w_v, rsem, ssem, a_rsem, a_ssem, lsem, bsem):
    nx, ny = dims
    kb, wcols = w.shape
    n = wcols // LANES
    nc = n - FIN
    full = n // 4
    half = kb // 2
    rows, kd = a_v.shape
    acols = kd // nx
    apiece = rows // A_PIECES

    x, y, c = lax.axis_index("co"), lax.axis_index("ri"), lax.axis_index("ro")
    xl, xr, xo = lax.rem(x + nx - 1, nx), lax.rem(x + 1, nx), lax.rem(x + 2, nx)
    yl, yr, yo = lax.rem(y + ny - 1, ny), lax.rem(y + 1, ny), lax.rem(y + 2, ny)

    barrier = pltpu.get_barrier_semaphore()
    peers = [{"co": xl}, {"co": xr}, {"co": xo}, {"ri": yl}, {"ri": yr}, {"ro": 1 - c}]
    for peer in peers:
        pl.semaphore_signal(barrier, inc=1, device_id=peer, device_id_type=MESH)
    pl.semaphore_wait(barrier, len(peers))

    def remote(src, dst, kind, j, dev):
        return pltpu.make_async_remote_copy(
            src_ref=src, dst_ref=dst, send_sem=ssem.at[kind, j], recv_sem=rsem.at[kind, j], device_id=dev, device_id_type=MESH
        )

    def arrived(ref, kind, j):
        remote(ref, ref, kind, j, {"ro": 1 - c}).wait_recv()

    def cols(j):
        return pl.ds(pl.multiple_of(j * LANES, LANES), LANES)

    def prow(is_full, part=0):
        size = kb if is_full else half
        return (pl.ds(0, size), pl.ds(0, size // 2), pl.ds(size // 2, size // 2))[part]

    def qrow(part=0):
        size = kb - half
        return (pl.ds(half, size), pl.ds(half, size // 2), pl.ds(half + size // 2, size // 2))[part]

    def s0p(j, t):
        src, dst = w.at[prow(t), cols(j)], g.at[j, c, y, x, prow(t), :]
        remote(src, dst, P1L, j, {"co": xr}).start()
        remote(src, dst, P1R, j, {"co": xl}).start()

    def s1p(j, t):
        arrived(g.at[j, c, y, xl, prow(t), :], P1L, j)
        up = g.at[j, c, y, xl, prow(t, 1), :]
        remote(up, up, P1U, j, {"co": xr}).start()
        arrived(g.at[j, c, y, xr, prow(t), :], P1R, j)
        down = g.at[j, c, y, xr, prow(t, 2), :]
        remote(down, down, P1D, j, {"co": xl}).start()

    def s2p(j, t):
        arrived(g.at[j, c, y, xo, prow(t, 1), :], P1U, j)
        arrived(g.at[j, c, y, xo, prow(t, 2), :], P1D, j)
        ref = g.at[j, c, y, :, prow(t), :]
        remote(ref, ref, P2L, j, {"ri": yr}).start()
        remote(ref, ref, P2R, j, {"ri": yl}).start()

    def s3p(j, t):
        arrived(g.at[j, c, yl, :, prow(t), :], P2L, j)
        up = g.at[j, c, yl, :, prow(t, 1), :]
        remote(up, up, P2U, j, {"ri": yr}).start()
        arrived(g.at[j, c, yr, :, prow(t), :], P2R, j)
        down = g.at[j, c, yr, :, prow(t, 2), :]
        remote(down, down, P2D, j, {"ri": yl}).start()

    def s4p(j, t):
        arrived(g.at[j, c, yo, :, prow(t, 1), :], P2U, j)
        arrived(g.at[j, c, yo, :, prow(t, 2), :], P2D, j)

    def s0q(j):
        src, dst = w.at[qrow(), cols(j)], g.at[j, c, y, x, qrow(), :]
        remote(src, dst, Q1L, j, {"ri": yr}).start()
        remote(src, dst, Q1R, j, {"ri": yl}).start()

    def s1q(j):
        arrived(g.at[j, c, yl, x, qrow(), :], Q1L, j)
        up = g.at[j, c, yl, x, qrow(1), :]
        remote(up, up, Q1U, j, {"ri": yr}).start()
        arrived(g.at[j, c, yr, x, qrow(), :], Q1R, j)
        down = g.at[j, c, yr, x, qrow(2), :]
        remote(down, down, Q1D, j, {"ri": yl}).start()

    def s2q(j):
        arrived(g.at[j, c, yo, x, qrow(1), :], Q1U, j)
        arrived(g.at[j, c, yo, x, qrow(2), :], Q1D, j)
        ref = g.at[j, c, :, x, qrow(), :]
        remote(ref, ref, Q2L, j, {"co": xr}).start()
        remote(ref, ref, Q2R, j, {"co": xl}).start()

    def s3q(j):
        arrived(g.at[j, c, :, xl, qrow(), :], Q2L, j)
        up = g.at[j, c, :, xl, qrow(1), :]
        remote(up, up, Q2U, j, {"co": xr}).start()
        arrived(g.at[j, c, :, xr, qrow(), :], Q2R, j)
        down = g.at[j, c, :, xr, qrow(2), :]
        remote(down, down, Q2D, j, {"co": xl}).start()

    def s4q(j):
        arrived(g.at[j, c, :, xo, qrow(1), :], Q2U, j)
        arrived(g.at[j, c, :, xo, qrow(2), :], Q2D, j)

    def own(j):
        return pltpu.make_async_copy(w_v.at[:, cols(j)], g.at[j, c, y, x], lsem.at[j])

    def die(j):
        return remote(g.at[j, c], g.at[j, c], DIE, j, {"ro": 1 - c})

    def a_copy(i, k, dev):
        src = act.at[pl.ds(pl.multiple_of(dev * rows + k * apiece, apiece), apiece), :]
        dst = a_v.at[pl.ds(pl.multiple_of(k * apiece, apiece), apiece), pl.ds(pl.multiple_of(x * acols, acols), acols)]
        return pltpu.make_async_remote_copy(
            src_ref=src, dst_ref=dst, send_sem=a_ssem.at[i], recv_sem=a_rsem.at[i], device_id={"co": dev}, device_id_type=MESH
        )

    def a_all(i, src_x):
        ref = a_v.at[:, pl.ds(pl.multiple_of(src_x * acols, acols), acols)]
        return pltpu.make_async_remote_copy(
            src_ref=ref, dst_ref=ref, send_sem=a_ssem.at[i], recv_sem=a_rsem.at[i], device_id={"ro": 1 - c}, device_id_type=MESH
        )

    own_a = pltpu.make_async_copy(
        act.at[pl.ds(pl.multiple_of(x * rows, rows), rows), :], a_v.at[:, pl.ds(pl.multiple_of(x * acols, acols), acols)], lsem.at[n]
    )
    own_w = pltpu.make_async_copy(w, w_v, lsem.at[n + 1])

    def load(j, slot):
        return loads(g, b_v, bsem, j, slot)

    def fetch(i, _):
        arrived(g.at[i, 1 - c], DIE, i)
        for cp in load(i, lax.rem(i, 2)):
            cp.start()
        return 0

    def use(i, _):
        slot = lax.rem(i, 2)

        @pl.when(i == 0)
        def _():
            own_a.wait()
            a_all(0, xl).wait_recv()
            a_all(1, xr).wait_recv()
            a_all(2, xo).wait_recv()

        @pl.when(i == nc - 1)
        def _():
            fetch(nc, 0)

        for cp in load(i, slot):
            cp.wait()
        multiply(a_v, b_v.at[slot], c_v, i)
        return 0

    def by_type(j, stage):
        pl.when((j >= 0) & (j < full))(lambda: stage(j, True))
        pl.when((j >= full) & (j < n))(lambda: stage(j, False))

    def if_q(j, stage):
        pl.when((j >= full) & (j < n))(lambda: stage(j))

    own_w.start()
    own_a.start()

    def start_own(j, _):
        own(j).start()
        return 0

    gap = 3
    lead = 3 * gap
    c_start = 7
    a_start = 3

    def finished(r):
        return jnp.clip(jnp.where(r <= n, r - gap, 2 * r - n - gap), 0, n)

    def progress(r):
        return jnp.clip(jnp.minimum(2 * (r - c_start), r - gap - 1), 0, nc)

    def last_hop(j, _):
        by_type(j, s4p)
        if_q(j, s4q)

        @pl.when(j < full)
        def _():
            die(j).start()

        @pl.when(j >= full)
        def _():
            die_part(j, g.at[j, c, yo, :, prow(False), :])
            die_part(j, g.at[j, c, :, xo, qrow(), :])

        return 0

    def die_part(j, ref):
        remote(ref, ref, DIE, j, {"ro": 1 - c}).start()

    def die_early(j):
        for b in (y, yl, yr):
            die_part(j, g.at[j, c, b, :, prow(False), :])
        for b in (x, xl, xr):
            die_part(j, g.at[j, c, :, b, qrow(), :])

    def turn(t, _):
        r = t - lead
        lax.fori_loop(progress(r), progress(r + 1), fetch, 0)
        by_type(r + 3 * gap, s0p)
        if_q(r + full + 3 * gap, s0q)

        @pl.when(t == 0)
        def _():
            own_w.wait()
            lax.fori_loop(0, n, start_own, 0)

        by_type(r + 2 * gap, s1p)
        if_q(r + full + 2 * gap, s1q)

        @pl.when((r >= -a_start) & (r < A_PIECES - a_start))
        def _():
            for i, dev in enumerate((xr, xl, xo)):
                a_copy(i, r + a_start, dev).start()

        @pl.when((r + gap >= 0) & (r + gap < n))
        def _():
            own(r + gap).wait()

        by_type(r + gap, s2p)
        if_q(r + gap, s2q)
        by_type(r, s3p)
        if_q(r, s3q)
        if_q(r, die_early)
        lax.fori_loop(finished(r), finished(r + 1), last_hop, 0)
        lax.fori_loop(progress(r), progress(r + 1), use, 0)
        return 0

    lax.fori_loop(0, nc + gap + 1 + lead, turn, 0)

    for cp in load(nc, nc % 2):
        cp.wait()
    arrived(g.at[n - 1, 1 - c], DIE, n - 1)
    for i, src_x in enumerate((xl, xr, xo)):
        a_all(i, src_x).wait_send()

    def sent(j, _):
        def p(j, t):
            for kind, ref in (
                (P1L, g.at[j, c, y, x, prow(t), :]),
                (P1R, g.at[j, c, y, x, prow(t), :]),
                (P1U, g.at[j, c, y, x, prow(t, 1), :]),
                (P1D, g.at[j, c, y, x, prow(t, 2), :]),
                (P2L, g.at[j, c, y, :, prow(t), :]),
                (P2R, g.at[j, c, y, :, prow(t), :]),
                (P2U, g.at[j, c, y, :, prow(t, 1), :]),
                (P2D, g.at[j, c, y, :, prow(t, 2), :]),
            ):
                remote(ref, ref, kind, j, {"ro": 1 - c}).wait_send()

        def q(j):
            for kind, ref in (
                (Q1L, g.at[j, c, y, x, qrow(), :]),
                (Q1R, g.at[j, c, y, x, qrow(), :]),
                (Q1U, g.at[j, c, y, x, qrow(1), :]),
                (Q1D, g.at[j, c, y, x, qrow(2), :]),
                (Q2L, g.at[j, c, :, x, qrow(), :]),
                (Q2R, g.at[j, c, :, x, qrow(), :]),
                (Q2U, g.at[j, c, :, x, qrow(1), :]),
                (Q2D, g.at[j, c, :, x, qrow(2), :]),
            ):
                remote(ref, ref, kind, j, {"ro": 1 - c}).wait_send()

        by_type(j, p)
        if_q(j, q)
        die(j).wait_send()
        return 0

    lax.fori_loop(0, n, sent, 0)


def loads(g, b_v, sem, j, slot):
    return [
        pltpu.make_async_copy(g.at[j, :, :, i], b_v.at[slot, :, :, :, pl.ds(i * LANES, LANES)], sem.at[slot, i])
        for i in range(g.shape[3])
    ]


def multiply_rows(a_v, b, c_v, j, m):
    nx = b.shape[-1] // LANES
    width = c_v.shape[-1] // nx
    r = pl.ds(pl.multiple_of(m * TILE, TILE), TILE)
    c = jnp.dot(a_v[r, :], b[...].reshape(a_v.shape[-1], nx * LANES), preferred_element_type=jnp.float32)
    for i in range(nx):
        col = pl.ds(pl.multiple_of(i * width + j * LANES, LANES), LANES)
        c_v[r, col] = c[:, i * LANES : (i + 1) * LANES].astype(c_v.dtype)


def multiply(a_v, b, c_v, j):
    def tile(m, _):
        multiply_rows(a_v, b, c_v, j, m)
        return 0

    lax.fori_loop(0, a_v.shape[0] // TILE, tile, 0)


def finish(a_v, b_v, c_v, g, out, last_v, d_v, bsem, csem, dsem):
    n, _, _, nx, _, _ = g.shape
    rows, nc = c_v.shape[0], n - FIN

    def stores(ref, first, count, k, size, sem):
        width = count * LANES
        r = pl.ds(pl.multiple_of(k * size, size), size)
        return [
            pltpu.make_async_copy(
                ref.at[r, pl.ds(i * width, width)], out.at[r, pl.ds((i * n + first) * LANES, width)], sem.at[k, i]
            )
            for i in range(nx)
        ]

    held = [cp for k in range(C_PARTS) for cp in stores(c_v, 0, nc, k, rows // C_PARTS, csem)]
    for cp in loads(g, last_v, bsem, n - 1, 0):
        cp.start()
    for cp in held:
        cp.start()

    multiply(a_v, b_v.at[nc % 2], d_v, 0)
    for cp in loads(g, last_v, bsem, n - 1, 0):
        cp.wait()

    def tile(m, _):
        multiply_rows(a_v, last_v.at[0], d_v, 1, m)
        for cp in stores(d_v, nc, FIN, m, TILE, dsem):
            cp.start()
        return 0

    lax.fori_loop(0, rows // TILE, tile, 0)
    for cp in held:
        cp.wait()
    for m in range(rows // TILE):
        for cp in stores(d_v, nc, FIN, m, TILE, dsem):
            cp.wait()


def solution(mesh):
    nx, ny, ncore = mesh.shape["co"], mesh.shape["ri"], mesh.shape["ro"]

    def local_block(act, w):
        kb, wcols = w.shape
        n = wcols // LANES
        rows, kd = act.shape[0] // nx, act.shape[1] * nx
        dt = act.dtype
        wide = nx * LANES
        any_spec = pl.BlockSpec(memory_space=pl.ANY)
        vmem_spec = pl.BlockSpec(memory_space=pltpu.VMEM)
        a_v, b_v, c_v, g = pl.pallas_call(
            functools.partial(kernel, (nx, ny)),
            name="gather_matmul",
            out_shape=(
                pltpu.VMEM((rows, kd), dt),
                pltpu.VMEM((2, ncore, ny, kb, wide), dt),
                pltpu.VMEM((rows, wide * (n - FIN)), dt),
                jax.ShapeDtypeStruct((n, ncore, ny, nx, kb, LANES), dt),
            ),
            in_specs=[any_spec] * 2,
            out_specs=(vmem_spec, vmem_spec, vmem_spec, any_spec),
            scratch_shapes=[
                pltpu.VMEM((kb, wcols), dt),
                pltpu.SemaphoreType.DMA((17, n)),
                pltpu.SemaphoreType.DMA((17, n)),
                pltpu.SemaphoreType.DMA((3,)),
                pltpu.SemaphoreType.DMA((3,)),
                pltpu.SemaphoreType.DMA((n + 2,)),
                pltpu.SemaphoreType.DMA((2, nx)),
            ],
            compiler_params=pltpu.CompilerParams(collective_id=0, has_side_effects=True, vmem_limit_bytes=12 << 20),
        )(act, w)
        held = [pltpu.with_memory_space_constraint(v, pltpu.VMEM) for v in (a_v, b_v, c_v)]
        return pl.pallas_call(
            finish,
            name="finish",
            out_shape=jax.ShapeDtypeStruct((rows, wcols * nx), dt),
            in_specs=[vmem_spec] * 3 + [any_spec],
            out_specs=any_spec,
            scratch_shapes=[
                pltpu.VMEM((1, ncore, ny, kb, wide), dt),
                pltpu.VMEM((rows, wide * FIN), dt),
                pltpu.SemaphoreType.DMA((1, nx)),
                pltpu.SemaphoreType.DMA((C_PARTS, nx)),
                pltpu.SemaphoreType.DMA((rows // TILE, nx)),
            ],
            compiler_params=pltpu.CompilerParams(vmem_limit_bytes=12 << 20),
        )(*held, g)

    return jax.shard_map(
        local_block,
        mesh=mesh,
        in_specs=(P(("dp", "ro", "ri"), "co"), P(("ro", "ri"), "co")),
        out_specs=P(("dp", "ro", "ri", "co"), None),
        check_vma=False,
    )
```

```python
import functools

import jax
import jax.numpy as jnp
from jax import lax
from jax.experimental import pallas as pl
from jax.experimental.pallas import tpu as pltpu
from jax.sharding import PartitionSpec as P

MESH = pl.DeviceIdType.MESH
LANES = 128
A_PIECES = 8
FIN = 2
AHEAD = 2
TILE = 512
C_PARTS = 4
P1L, P1R, P1U, P1D, P2L, P2R, P2U, P2D, Q1L, Q1R, Q1U, Q1D, Q2L, Q2R, Q2U, Q2D, DIE = range(17)


def kernel(dims, act, w, a_v, b_v, c_v, g, w_v, rsem, ssem, a_rsem, a_ssem, lsem, bsem):
    nx, ny = dims
    kb, wcols = w.shape
    n = wcols // LANES
    nc = n - FIN
    full = n // 4
    half = kb // 2
    rows, kd = a_v.shape
    acols = kd // nx
    apiece = rows // A_PIECES

    x, y, c = lax.axis_index("co"), lax.axis_index("ri"), lax.axis_index("ro")
    xl, xr, xo = lax.rem(x + nx - 1, nx), lax.rem(x + 1, nx), lax.rem(x + 2, nx)
    yl, yr, yo = lax.rem(y + ny - 1, ny), lax.rem(y + 1, ny), lax.rem(y + 2, ny)

    barrier = pltpu.get_barrier_semaphore()
    peers = [{"co": xl}, {"co": xr}, {"co": xo}, {"ri": yl}, {"ri": yr}, {"ro": 1 - c}]
    for peer in peers:
        pl.semaphore_signal(barrier, inc=1, device_id=peer, device_id_type=MESH)
    pl.semaphore_wait(barrier, len(peers))

    def remote(src, dst, kind, j, dev):
        return pltpu.make_async_remote_copy(
            src_ref=src, dst_ref=dst, send_sem=ssem.at[kind, j], recv_sem=rsem.at[kind, j], device_id=dev, device_id_type=MESH
        )

    def arrived(ref, kind, j):
        remote(ref, ref, kind, j, {"ro": 1 - c}).wait_recv()

    def cols(j):
        return pl.ds(pl.multiple_of(j * LANES, LANES), LANES)

    def prow(is_full, part=0):
        size = kb if is_full else half
        return (pl.ds(0, size), pl.ds(0, size // 2), pl.ds(size // 2, size // 2))[part]

    def qrow(part=0):
        size = kb - half
        return (pl.ds(half, size), pl.ds(half, size // 2), pl.ds(half + size // 2, size // 2))[part]

    def s0p(j, t):
        src, dst = w.at[prow(t), cols(j)], g.at[j, c, y, x, prow(t), :]
        remote(src, dst, P1L, j, {"co": xr}).start()
        remote(src, dst, P1R, j, {"co": xl}).start()

    def s1p(j, t):
        arrived(g.at[j, c, y, xl, prow(t), :], P1L, j)
        up = g.at[j, c, y, xl, prow(t, 1), :]
        remote(up, up, P1U, j, {"co": xr}).start()
        arrived(g.at[j, c, y, xr, prow(t), :], P1R, j)
        down = g.at[j, c, y, xr, prow(t, 2), :]
        remote(down, down, P1D, j, {"co": xl}).start()

    def s2p(j, t):
        arrived(g.at[j, c, y, xo, prow(t, 1), :], P1U, j)
        arrived(g.at[j, c, y, xo, prow(t, 2), :], P1D, j)
        ref = g.at[j, c, y, :, prow(t), :]
        remote(ref, ref, P2L, j, {"ri": yr}).start()
        remote(ref, ref, P2R, j, {"ri": yl}).start()

    def s3p(j, t):
        arrived(g.at[j, c, yl, :, prow(t), :], P2L, j)
        up = g.at[j, c, yl, :, prow(t, 1), :]
        remote(up, up, P2U, j, {"ri": yr}).start()
        arrived(g.at[j, c, yr, :, prow(t), :], P2R, j)
        down = g.at[j, c, yr, :, prow(t, 2), :]
        remote(down, down, P2D, j, {"ri": yl}).start()

    def s4p(j, t):
        arrived(g.at[j, c, yo, :, prow(t, 1), :], P2U, j)
        arrived(g.at[j, c, yo, :, prow(t, 2), :], P2D, j)

    def s0q(j):
        src, dst = w.at[qrow(), cols(j)], g.at[j, c, y, x, qrow(), :]
        remote(src, dst, Q1L, j, {"ri": yr}).start()
        remote(src, dst, Q1R, j, {"ri": yl}).start()

    def s1q(j):
        arrived(g.at[j, c, yl, x, qrow(), :], Q1L, j)
        up = g.at[j, c, yl, x, qrow(1), :]
        remote(up, up, Q1U, j, {"ri": yr}).start()
        arrived(g.at[j, c, yr, x, qrow(), :], Q1R, j)
        down = g.at[j, c, yr, x, qrow(2), :]
        remote(down, down, Q1D, j, {"ri": yl}).start()

    def s2q(j):
        arrived(g.at[j, c, yo, x, qrow(1), :], Q1U, j)
        arrived(g.at[j, c, yo, x, qrow(2), :], Q1D, j)
        ref = g.at[j, c, :, x, qrow(), :]
        remote(ref, ref, Q2L, j, {"co": xr}).start()
        remote(ref, ref, Q2R, j, {"co": xl}).start()

    def s3q(j):
        arrived(g.at[j, c, :, xl, qrow(), :], Q2L, j)
        up = g.at[j, c, :, xl, qrow(1), :]
        remote(up, up, Q2U, j, {"co": xr}).start()
        arrived(g.at[j, c, :, xr, qrow(), :], Q2R, j)
        down = g.at[j, c, :, xr, qrow(2), :]
        remote(down, down, Q2D, j, {"co": xl}).start()

    def s4q(j):
        arrived(g.at[j, c, :, xo, qrow(1), :], Q2U, j)
        arrived(g.at[j, c, :, xo, qrow(2), :], Q2D, j)

    def own(j):
        return pltpu.make_async_copy(w_v.at[:, cols(j)], g.at[j, c, y, x], lsem.at[j])

    def die(j):
        return remote(g.at[j, c], g.at[j, c], DIE, j, {"ro": 1 - c})

    def a_copy(i, k, dev):
        src = act.at[pl.ds(pl.multiple_of(dev * rows + k * apiece, apiece), apiece), :]
        dst = a_v.at[pl.ds(pl.multiple_of(k * apiece, apiece), apiece), pl.ds(pl.multiple_of(x * acols, acols), acols)]
        return pltpu.make_async_remote_copy(
            src_ref=src, dst_ref=dst, send_sem=a_ssem.at[i], recv_sem=a_rsem.at[i], device_id={"co": dev}, device_id_type=MESH
        )

    def a_all(i, src_x):
        ref = a_v.at[:, pl.ds(pl.multiple_of(src_x * acols, acols), acols)]
        return pltpu.make_async_remote_copy(
            src_ref=ref, dst_ref=ref, send_sem=a_ssem.at[i], recv_sem=a_rsem.at[i], device_id={"ro": 1 - c}, device_id_type=MESH
        )

    own_a = pltpu.make_async_copy(
        act.at[pl.ds(pl.multiple_of(x * rows, rows), rows), :], a_v.at[:, pl.ds(pl.multiple_of(x * acols, acols), acols)], lsem.at[n]
    )
    own_w = pltpu.make_async_copy(w, w_v, lsem.at[n + 1])

    def load(j, slot):
        return loads(g, b_v, bsem, j, slot)

    def fetch(i, _):
        arrived(g.at[i, 1 - c], DIE, i)
        for cp in load(i, lax.rem(i, 2)):
            cp.start()
        return 0

    def use(i, _):
        slot = lax.rem(i, 2)

        @pl.when(i == 0)
        def _():
            own_a.wait()
            a_all(0, xl).wait_recv()
            a_all(1, xr).wait_recv()
            a_all(2, xo).wait_recv()

        for cp in load(i, slot):
            cp.wait()

        @pl.when(i >= nc - AHEAD)
        def _():
            fetch(i + 1, 0)

        multiply(a_v, b_v.at[slot], c_v, i)
        return 0

    def by_type(j, stage):
        pl.when((j >= 0) & (j < full))(lambda: stage(j, True))
        pl.when((j >= full) & (j < n))(lambda: stage(j, False))

    def if_q(j, stage):
        pl.when((j >= full) & (j < n))(lambda: stage(j))

    own_w.start()
    own_a.start()

    def start_own(j, _):
        own(j).start()
        return 0

    gap = 3
    lead = 3 * gap
    c_start = 7
    early = nc - AHEAD + 1
    a_start = 3

    def finished(r):
        return jnp.clip(jnp.where(r <= n, r - gap, 2 * r - n - gap), 0, n)

    def progress(r):
        return jnp.clip(jnp.minimum(2 * (r - c_start), r - gap - 1), 0, nc)

    def last_hop(j, _):
        by_type(j, s4p)
        if_q(j, s4q)

        @pl.when(j < full)
        def _():
            die(j).start()

        @pl.when(j >= full)
        def _():
            die_part(j, g.at[j, c, yo, :, prow(False), :])
            die_part(j, g.at[j, c, :, xo, qrow(), :])

        return 0

    def die_part(j, ref):
        remote(ref, ref, DIE, j, {"ro": 1 - c}).start()

    def die_early(j):
        for b in (y, yl, yr):
            die_part(j, g.at[j, c, b, :, prow(False), :])
        for b in (x, xl, xr):
            die_part(j, g.at[j, c, :, b, qrow(), :])

    def turn(t, _):
        r = t - lead
        lax.fori_loop(jnp.minimum(progress(r), early), jnp.minimum(progress(r + 1), early), fetch, 0)
        by_type(r + 3 * gap, s0p)
        if_q(r + full + 3 * gap, s0q)

        @pl.when(t == 0)
        def _():
            own_w.wait()
            lax.fori_loop(0, n, start_own, 0)

        by_type(r + 2 * gap, s1p)
        if_q(r + full + 2 * gap, s1q)

        @pl.when((r >= -a_start) & (r < A_PIECES - a_start))
        def _():
            for i, dev in enumerate((xr, xl, xo)):
                a_copy(i, r + a_start, dev).start()

        @pl.when((r + gap >= 0) & (r + gap < n))
        def _():
            own(r + gap).wait()

        by_type(r + gap, s2p)
        if_q(r + gap, s2q)
        by_type(r, s3p)
        if_q(r, s3q)
        if_q(r, die_early)
        lax.fori_loop(finished(r), finished(r + 1), last_hop, 0)
        lax.fori_loop(progress(r), progress(r + 1), use, 0)
        return 0

    lax.fori_loop(0, nc + gap + 1 + lead, turn, 0)

    for cp in load(nc, nc % 2):
        cp.wait()
    arrived(g.at[n - 1, 1 - c], DIE, n - 1)
    for i, src_x in enumerate((xl, xr, xo)):
        a_all(i, src_x).wait_send()

    def sent(j, _):
        def p(j, t):
            for kind, ref in (
                (P1L, g.at[j, c, y, x, prow(t), :]),
                (P1R, g.at[j, c, y, x, prow(t), :]),
                (P1U, g.at[j, c, y, x, prow(t, 1), :]),
                (P1D, g.at[j, c, y, x, prow(t, 2), :]),
                (P2L, g.at[j, c, y, :, prow(t), :]),
                (P2R, g.at[j, c, y, :, prow(t), :]),
                (P2U, g.at[j, c, y, :, prow(t, 1), :]),
                (P2D, g.at[j, c, y, :, prow(t, 2), :]),
            ):
                remote(ref, ref, kind, j, {"ro": 1 - c}).wait_send()

        def q(j):
            for kind, ref in (
                (Q1L, g.at[j, c, y, x, qrow(), :]),
                (Q1R, g.at[j, c, y, x, qrow(), :]),
                (Q1U, g.at[j, c, y, x, qrow(1), :]),
                (Q1D, g.at[j, c, y, x, qrow(2), :]),
                (Q2L, g.at[j, c, :, x, qrow(), :]),
                (Q2R, g.at[j, c, :, x, qrow(), :]),
                (Q2U, g.at[j, c, :, x, qrow(1), :]),
                (Q2D, g.at[j, c, :, x, qrow(2), :]),
            ):
                remote(ref, ref, kind, j, {"ro": 1 - c}).wait_send()

        by_type(j, p)
        if_q(j, q)
        die(j).wait_send()
        return 0

    lax.fori_loop(0, n, sent, 0)


def loads(g, b_v, sem, j, slot):
    return [
        pltpu.make_async_copy(g.at[j, :, :, i], b_v.at[slot, :, :, :, pl.ds(i * LANES, LANES)], sem.at[slot, i])
        for i in range(g.shape[3])
    ]


def multiply_rows(a_v, b, c_v, j, m):
    nx = b.shape[-1] // LANES
    width = c_v.shape[-1] // nx
    r = pl.ds(pl.multiple_of(m * TILE, TILE), TILE)
    c = jnp.dot(a_v[r, :], b[...].reshape(a_v.shape[-1], nx * LANES), preferred_element_type=jnp.float32)
    for i in range(nx):
        col = pl.ds(pl.multiple_of(i * width + j * LANES, LANES), LANES)
        c_v[r, col] = c[:, i * LANES : (i + 1) * LANES].astype(c_v.dtype)


def multiply(a_v, b, c_v, j):
    def tile(m, _):
        multiply_rows(a_v, b, c_v, j, m)
        return 0

    lax.fori_loop(0, a_v.shape[0] // TILE, tile, 0)


def finish(a_v, b_v, c_v, g, out, last_v, d_v, bsem, csem, dsem):
    n, _, _, nx, _, _ = g.shape
    rows, nc = c_v.shape[0], n - FIN

    def stores(ref, first, count, k, size, sem):
        width = count * LANES
        r = pl.ds(pl.multiple_of(k * size, size), size)
        return [
            pltpu.make_async_copy(
                ref.at[r, pl.ds(i * width, width)], out.at[r, pl.ds((i * n + first) * LANES, width)], sem.at[k, i]
            )
            for i in range(nx)
        ]

    held = [cp for k in range(C_PARTS) for cp in stores(c_v, 0, nc, k, rows // C_PARTS, csem)]
    for cp in loads(g, last_v, bsem, n - 1, 0):
        cp.start()
    for cp in held:
        cp.start()

    multiply(a_v, b_v.at[nc % 2], d_v, 0)
    for cp in loads(g, last_v, bsem, n - 1, 0):
        cp.wait()

    def tile(m, _):
        multiply_rows(a_v, last_v.at[0], d_v, 1, m)
        for cp in stores(d_v, nc, FIN, m, TILE, dsem):
            cp.start()
        return 0

    lax.fori_loop(0, rows // TILE, tile, 0)
    for cp in held:
        cp.wait()
    for m in range(rows // TILE):
        for cp in stores(d_v, nc, FIN, m, TILE, dsem):
            cp.wait()


def solution(mesh):
    nx, ny, ncore = mesh.shape["co"], mesh.shape["ri"], mesh.shape["ro"]

    def local_block(act, w):
        kb, wcols = w.shape
        n = wcols // LANES
        rows, kd = act.shape[0] // nx, act.shape[1] * nx
        dt = act.dtype
        wide = nx * LANES
        any_spec = pl.BlockSpec(memory_space=pl.ANY)
        vmem_spec = pl.BlockSpec(memory_space=pltpu.VMEM)
        a_v, b_v, c_v, g = pl.pallas_call(
            functools.partial(kernel, (nx, ny)),
            name="gather_matmul",
            out_shape=(
                pltpu.VMEM((rows, kd), dt),
                pltpu.VMEM((2, ncore, ny, kb, wide), dt),
                pltpu.VMEM((rows, wide * (n - FIN)), dt),
                jax.ShapeDtypeStruct((n, ncore, ny, nx, kb, LANES), dt),
            ),
            in_specs=[any_spec] * 2,
            out_specs=(vmem_spec, vmem_spec, vmem_spec, any_spec),
            scratch_shapes=[
                pltpu.VMEM((kb, wcols), dt),
                pltpu.SemaphoreType.DMA((17, n)),
                pltpu.SemaphoreType.DMA((17, n)),
                pltpu.SemaphoreType.DMA((3,)),
                pltpu.SemaphoreType.DMA((3,)),
                pltpu.SemaphoreType.DMA((n + 2,)),
                pltpu.SemaphoreType.DMA((2, nx)),
            ],
            compiler_params=pltpu.CompilerParams(collective_id=0, has_side_effects=True, vmem_limit_bytes=12 << 20),
        )(act, w)
        held = [pltpu.with_memory_space_constraint(v, pltpu.VMEM) for v in (a_v, b_v, c_v)]
        return pl.pallas_call(
            finish,
            name="finish",
            out_shape=jax.ShapeDtypeStruct((rows, wcols * nx), dt),
            in_specs=[vmem_spec] * 3 + [any_spec],
            out_specs=any_spec,
            scratch_shapes=[
                pltpu.VMEM((1, ncore, ny, kb, wide), dt),
                pltpu.VMEM((rows, wide * FIN), dt),
                pltpu.SemaphoreType.DMA((1, nx)),
                pltpu.SemaphoreType.DMA((C_PARTS, nx)),
                pltpu.SemaphoreType.DMA((rows // TILE, nx)),
            ],
            compiler_params=pltpu.CompilerParams(vmem_limit_bytes=12 << 20),
        )(*held, g)

    return jax.shard_map(
        local_block,
        mesh=mesh,
        in_specs=(P(("dp", "ro", "ri"), "co"), P(("ro", "ri"), "co")),
        out_specs=P(("dp", "ro", "ri", "co"), None),
        check_vma=False,
    )
```
